32 devices in a mesh: section: 2 (over core), vocab: 16 (over z, y, x).
Axes of the slice: x: 2, y: 2, z: 4, core: 2. Of those that a mesh axis runs over, the one named last changes fastest.
Arguments:
- hidden_in: bfloat16 [2, 256, 7168], P(None, ('section', 'vocab')), may hold values from -6 to 6
- gain_ffn: float32 [7168], replicated, may hold values from 0.4 to 1.6
- w_gate: bfloat16 [7168, 18432], P(None, ('section', 'vocab')), may hold values from -0.0625 to 0.0625
- w_up: bfloat16 [7168, 18432], P(None, ('section', 'vocab')), may hold values from -0.0625 to 0.0625
- w_down: bfloat16 [18432, 7168], P(('section', 'vocab')), may hold values from -0.046875 to 0.046875
- gain_final: float32 [7168], replicated, may hold values from 0.4 to 1.6
- head_weight: bfloat16 [7168, 129280], P(None, ('section', 'vocab')), may hold values from -4.5 to 4.5
- sampled_ids: int32 [2, 256], replicated, may hold values from 0 to 129279
- seq_ids: int32 [2, 256], P(None, ('section', 'vocab')), may hold values from 0 to 7, never falling along the last dimension, each value on 1 to 128 neighbouring positions
Outputs:
- token_logprob: float32 [2, 256], P(None, ('section', 'vocab'))
- log_norm: float32 [2, 256], P(None, ('section', 'vocab'))
- top_mass: float32 [2, 256], P(None, ('section', 'vocab'))
- seq_logprob: float32 [2, 8], replicated
The draws below stay inside these ranges and needn't reach their ends.
All inputs are finite; a program needn't handle non-finite values.
Results may differ from the reference program's by a relative error of at most 0.006.
Values may be sent and summed in bfloat16 or wider, within the bound.
No kernel may reach another device: no remote copies, remote signals or barrier semaphores. Data moves between devices by JAX's collectives and lax.ppermute only.
A program may use at most 192 MiB of HBM per device.

```python
import math
import jax
import jax.numpy as jnp
import numpy as np
from jax import lax

D = 7168
FF = 18432
VOCAB = 129280
MB = 2
MB_TOK = 256
SEQS = 8
TOPK = 20


def draw_head_weight(key, part):
    base_key = jax.random.fold_in(key, 11)
    key_scale, key_entries = jax.random.split(base_key, 2)
    column_scale = jnp.exp(jax.random.uniform(key_scale, (1, VOCAB), jnp.float32, math.log(0.7), math.log(7.0)))
    entries = jax.random.normal(key_entries, (D, VOCAB), jnp.float32)
    weight = entries * column_scale / math.sqrt(D)
    return jnp.clip(weight, -4.5, 4.5).astype(jnp.bfloat16)


def place_ends(array, stream_key, least, top_value):
    extent = array.shape
    spot = [jax.random.randint(jax.random.fold_in(stream_key, axis), (), 0, extent[axis]) for axis in range(len(extent))]
    array = array.at[tuple(spot)].set(least)
    longest = extent.index(max(extent))
    spot[longest] = (spot[longest] + 1) % extent[longest]
    return array.at[tuple(spot)].set(top_value)


def steps_of(rng, extent, shards, least, high):
    gain, own = 1.0, jax.random.fold_in(rng, 6)
    for position, blocks in shards:
        draws = jnp.exp(jax.random.uniform(jax.random.fold_in(own, position), (blocks,), jnp.float32, least / len(shards), high / len(shards)))
        gain = gain * jnp.repeat(draws, extent[position] // blocks).reshape([-1 if axis == position else 1 for axis in range(len(extent))])
    return gain


def split_up(number_of, total, limit, skew):
    weights = [(1 << 20) // math.isqrt(rank ** skew) + 1 for rank in range(2, number_of + 1)]
    surplus, counts = total - limit - (number_of - 1), [1] * (number_of - 1)
    while surplus > 0:
        candidates = [i for i in range(number_of - 1) if counts[i] < limit]
        pool, left = sum([weights[i] for i in candidates]), surplus
        for i in candidates:
            more = min(limit - counts[i], max(1, left * weights[i] // pool), surplus)
            counts[i] = counts[i] + more
            surplus = surplus - more
    return np.array([limit] + counts)


def ragged_sizes(key, number_of, total, most, slope):
    if number_of == 2:
        one = jax.random.randint(key, (), max(1, total - most), min(most, total - 1) + 1)
        return jnp.stack([one, total - one])
    lengths = jnp.asarray(split_up(number_of, total, most, slope), jnp.int32)
    couples = (number_of - 1) // 2
    donor, taker = lengths[1:1 + 2 * couples:2], lengths[2:2 + 2 * couples:2]
    margin = jnp.minimum(donor - 1, most - taker)
    passed = jax.random.randint(jax.random.fold_in(key, 1), (couples,), 0, 1 << 20) % (margin + 1)
    lengths = lengths.at[1:1 + 2 * couples:2].set(donor - passed).at[2:2 + 2 * couples:2].set(taker + passed)
    return lengths[jax.random.permutation(jax.random.fold_in(key, 2), number_of)]


def gaussian(own_key, extent, width, limit, cuts=(), kind=jnp.bfloat16):
    values = jax.random.normal(own_key, extent, jnp.float32) * width
    if len(cuts) > 0:
        values = steps_of(own_key, extent, cuts, -0.22, 0.18) * values
    return jnp.clip(values, min=-limit, max=limit).astype(kind)


def setup_inputs(seed: int = 0) -> dict:
    streams_of = jax.random.split(jax.random.key(seed), 10)
    hidden_in = gaussian(streams_of[0], (MB, MB_TOK, D), 1.0, 6.0, ((1, 32),))
    gain_ffn = jnp.clip(1.0 + 0.12 * jax.random.normal(streams_of[1], (D,), jnp.float32), 0.4, 1.6)
    w_gate = gaussian(streams_of[2], (D, FF), D ** -0.5, 0.0625, ((1, 32),))
    w_up = gaussian(streams_of[3], (D, FF), D ** -0.5, 0.0625, ((1, 32),))
    w_down = gaussian(streams_of[4], (FF, D), FF ** -0.5, 0.046875, ((0, 32),))
    gain_final = jnp.clip(1.0 + 0.12 * jax.random.normal(streams_of[5], (D,), jnp.float32), 0.4, 1.6)
    head_weight = draw_head_weight(jax.random.fold_in(streams_of[9], 71), 0)
    sampled_ids = place_ends(jax.random.randint(streams_of[7], (MB, MB_TOK), 0, VOCAB), jax.random.fold_in(streams_of[7], 1), 0, VOCAB - 1).astype(jnp.int32)
    seq_ids = jax.vmap(lambda own: jnp.searchsorted(jnp.cumsum(ragged_sizes(own, SEQS, MB_TOK, MB_TOK // 2, 2)), jnp.arange(MB_TOK), side="right"))(jax.random.split(streams_of[8], MB)).reshape((MB, MB_TOK)).astype(jnp.int32)
    return {"hidden_in": hidden_in, "gain_ffn": gain_ffn, "w_gate": w_gate, "w_up": w_up, "w_down": w_down, "gain_final": gain_final, "head_weight": head_weight, "sampled_ids": sampled_ids, "seq_ids": seq_ids}


epsilon = 1e-06

def rms_norm(values, scale_gain):
    wide = values.astype(jnp.float32)
    square_mean = lax.optimization_barrier(jnp.mean(wide * wide, axis=-1, keepdims=True))
    return (wide * lax.rsqrt(square_mean + epsilon) * scale_gain).astype(jnp.bfloat16)

def largest(values):
    return lax.sort(values, dimension=values.ndim - 1)[..., -TOPK:]

def reference(hidden_in, gain_ffn, w_gate, w_up, w_down, gain_final, head_weight, sampled_ids, seq_ids):

    def score_batch(record):
        states, token_ids, segment_ids = record
        normed = rms_norm(states, gain_ffn)
        gate_proj = jnp.dot(normed, w_gate, preferred_element_type=jnp.float32)
        up_proj = jnp.dot(normed, w_up, preferred_element_type=jnp.float32)
        hidden_act = (jax.nn.silu(gate_proj) * up_proj).astype(jnp.bfloat16)
        branch = jnp.dot(hidden_act, w_down, preferred_element_type=jnp.float32)
        residual = (states.astype(jnp.float32) + branch).astype(jnp.bfloat16)
        scaled = rms_norm(residual, gain_final)
        logits = jnp.dot(scaled, head_weight, preferred_element_type=jnp.float32)
        peak_value = lax.optimization_barrier(jnp.max(logits, axis=1))
        log_norm = peak_value + jnp.log(lax.optimization_barrier(jnp.sum(jnp.exp(logits - peak_value[:, None]), axis=1)))
        sampled_logit = jnp.take_along_axis(logits, token_ids[:, None].astype(jnp.int32), axis=1)[:, 0]
        token_logprob = sampled_logit - log_norm
        leaders = largest(logits)
        top_mass = lax.optimization_barrier(jnp.sum(jnp.exp(leaders - log_norm[:, None]), axis=1))
        onehot = (segment_ids[:, None] == jnp.arange(SEQS, dtype=jnp.int32)[None, :]).astype(jnp.float32)
        seq_total = lax.optimization_barrier(jnp.sum(token_logprob[:, None] * onehot, axis=0))
        return (token_logprob, log_norm, top_mass, seq_total)
    token_logprob, log_norm, top_mass, seq_logprob = lax.map(score_batch, (hidden_in, sampled_ids, seq_ids))
    return (token_logprob, log_norm, top_mass, seq_logprob)
```

```python
import functools

import jax
import jax.numpy as jnp
from jax import lax
from jax.experimental import pallas as pl
from jax.experimental.pallas import tpu as pltpu
from jax.sharding import PartitionSpec as P

SEQS = 8
TOPK = 20
LANES = 128
NET = 32
AXES = ("section", "vocab")
epsilon = 1e-06


def rms_norm(wide, gain):
    square_mean = jnp.mean(wide * wide, axis=-1, keepdims=True)
    return (wide * lax.rsqrt(square_mean + epsilon) * gain).astype(jnp.bfloat16)


def step_masks(size):
    bits = [1 << b for b in reversed(range(size.bit_length() - 1))]
    return bits, bits[:-2] + [bits[-1], bits[-2]]


def step_perms(size):
    first, second = step_masks(size)
    return [
        [(s * size + i, s * size + (i ^ mask)) for s, mask in enumerate(pair) for i in range(size)]
        for pair in zip(first, second)
    ]


def core_perm(size):
    return [(s * size + i, (1 - s) * size + i) for s in range(2) for i in range(size)]


def gather_rows(rows, size):
    held = rows
    for perm in step_perms(size):
        held = jnp.concatenate([held, lax.ppermute(held, AXES, perm)], axis=0)
    return held, lax.ppermute(held, AXES, core_perm(size))


def scatter_sum(near, far, size):
    held = near + lax.ppermute(far, AXES, core_perm(size))
    perms = step_perms(size)
    for perm in reversed(perms[1:]):
        half = held.shape[0] // 2
        held = held[:half] + lax.ppermute(held[half:], AXES, perm)
    half = held.shape[0] // 2
    return held[:half].astype(jnp.float32) + lax.ppermute(held[half:], AXES, perms[0]).astype(jnp.float32)


def block_owner(size, section, place):
    tables = []
    for masks in step_masks(size):
        table = []
        for q in range(size):
            mask = 0
            for j, m in enumerate(masks):
                if q >> j & 1:
                    mask ^= m
            table.append(mask)
        tables.append(jnp.array(table, jnp.int32))
    mine = jnp.where(section == 0, tables[0], tables[1])
    other = jnp.where(section == 0, tables[1], tables[0])
    return jnp.concatenate([section * size + (place ^ mine), (1 - section) * size + (place ^ other)])


def turned_dot(a, b):
    return lax.dot_general(a, b, (((1,), (1,)), ((), ())), preferred_element_type=jnp.float32)


def ffn_kernel(near_ref, far_ref, wg_ref, wu_ref, wd_ref, near_out, far_out, x_ref, turned_ref, h_ref, *, steps):
    i = pl.program_id(0)
    half = near_ref.shape[0]
    tile = wg_ref.shape[0]

    @pl.when(i == 0)
    def _():
        x_ref[:half] = near_ref[...]
        x_ref[half:] = far_ref[...]

    @pl.when(i < steps)
    def _():
        gate = turned_dot(wg_ref[...], x_ref[...])
        up = turned_dot(wu_ref[...], x_ref[...])
        turned_ref[pl.ds(pl.multiple_of(i * tile, tile), tile), :] = gate / (1.0 + jnp.exp(-gate)) * up

    @pl.when(i == steps - 1)
    def _():
        h_ref[...] = turned_ref[...].T.astype(jnp.bfloat16)

    @pl.when(i >= steps)
    def _():
        part = jnp.dot(h_ref[...], wd_ref[...], preferred_element_type=jnp.float32).astype(near_out.dtype)
        near_out[...] = part[:half]
        far_out[...] = part[half:]


def ffn(near, far, w_gate, w_up, w_down):
    half, width = near.shape
    rows = 2 * half
    hidden = w_gate.shape[1]
    tile = hidden // 2 if hidden % 32 == 0 else hidden
    block = 1792 if width % 1792 == 0 else width
    steps = hidden // tile

    def first(i):
        return jnp.minimum(i, steps - 1)

    def second(i):
        return jnp.maximum(i - steps, 0)

    part = jax.ShapeDtypeStruct((half, width), jnp.bfloat16)
    return pl.pallas_call(
        functools.partial(ffn_kernel, steps=steps),
        grid=(steps + width // block,),
        in_specs=[
            pl.BlockSpec((half, width), lambda i: (0, 0)),
            pl.BlockSpec((half, width), lambda i: (0, 0)),
            pl.BlockSpec((tile, width), lambda i: (first(i), 0)),
            pl.BlockSpec((tile, width), lambda i: (first(i), 0)),
            pl.BlockSpec((hidden, block), lambda i: (0, second(i))),
        ],
        out_specs=[pl.BlockSpec((half, block), lambda i: (0, second(i)))] * 2,
        out_shape=(part, part),
        scratch_shapes=[
            pltpu.VMEM((rows, width), jnp.bfloat16),
            pltpu.VMEM((hidden, rows), jnp.float32),
            pltpu.VMEM((rows, hidden), jnp.bfloat16),
        ],
        cost_estimate=pl.CostEstimate(
            flops=6 * rows * width * hidden, bytes_accessed=2 * width * (3 * hidden + 2 * rows), transcendentals=0
        ),
        name="ffn",
    )(near, far, w_gate.T, w_up.T, w_down)


def pair(values, i, j):
    a, b = values[i], values[j]
    if b is None:
        return
    if a is None:
        values[i], values[j] = b, None
    else:
        values[i], values[j] = jnp.maximum(a, b), jnp.minimum(a, b)


def sort_net(values):
    values = list(values) + [None] * (NET - len(values))
    p = 1
    while p < NET:
        k = p
        while k >= 1:
            for j in range(k % p, NET - k, 2 * k):
                for i in range(min(k, NET - j - k)):
                    if (i + j) // (2 * p) == (i + j + k) // (2 * p):
                        pair(values, i + j, i + j + k)
            k //= 2
        p *= 2
    return values[:TOPK]


def merge_net(a, b):
    a = list(a) + [None] * (NET - len(a))
    b = list(b) + [None] * (NET - len(b))
    c = []
    for x, y in zip(a, reversed(b)):
        c.append(y if x is None else x if y is None else jnp.maximum(x, y))
    k = NET // 2
    while k >= 1:
        for base in range(0, NET, 2 * k):
            for i in range(base, base + k):
                pair(c, i, i + k)
        k //= 2
    return c[:TOPK]


def head_kernel(owner_ref, near_ref, far_ref, w_ref, ids_ref, out_ref, x_ref, logits_ref, stat_ref, *, steps, width):
    i = pl.program_id(0)
    half = near_ref.shape[0]
    tile = w_ref.shape[0]

    @pl.when(i == 0)
    def _():
        x_ref[:half] = near_ref[...]
        x_ref[half:] = far_ref[...]

    logits_ref[pl.ds(pl.multiple_of(i * tile, tile), tile), :] = turned_dot(w_ref[...], x_ref[...])

    @pl.when(i == steps - 1)
    def _():
        rows = x_ref.shape[0]
        each = out_ref.shape[1]
        whole = width // (8 * NET)
        sub = lax.broadcasted_iota(jnp.int32, (8, LANES), 0)

        def load(start, lanes):
            return logits_ref[pl.ds(start, 8), lanes]

        def rest(lanes):
            values = []
            for start in range(whole * 8 * NET, width, 8):
                value = load(start, lanes)
                if start + 8 > width:
                    value = jnp.where(sub < width - start, value, -jnp.inf)
                values.append(value)
            return values

        stat_ref[...] = jnp.zeros_like(stat_ref)
        for lane in range(0, rows, LANES):
            lanes = slice(lane, lane + LANES)

            def collect(g, best):
                start = pl.multiple_of(g * 8 * NET, 8 * NET)
                return tuple(merge_net(best, sort_net([load(start + 8 * j, lanes) for j in range(NET)])))

            low = jnp.full((8, LANES), -jnp.inf, jnp.float32)
            best = list(lax.fori_loop(0, whole, collect, (low,) * TOPK))
            tail = rest(lanes)
            if tail:
                ranked = sort_net(tail)
                best = merge_net(best, [r for r in ranked if r is not None])
            for shift in (4, 2, 1):
                best = merge_net(best, [pltpu.roll(b, shift, 0) for b in best])
            peak = best[0]
            wanted = jnp.broadcast_to(ids_ref[:, lanes], (8, LANES)) - sub

            def scan(value, start, total, found):
                total = total + jnp.exp(value - peak)
                return total, found + jnp.where(wanted == start, value, 0.0)

            def sweep(g, carry):
                start = pl.multiple_of(g * 8 * NET, 8 * NET)
                totals, founds = list(carry[:4]), list(carry[4:])
                for j in range(NET):
                    t, f = scan(load(start + 8 * j, lanes), start + 8 * j, totals[j % 4], founds[j % 4])
                    totals[j % 4], founds[j % 4] = t, f
                return tuple(totals) + tuple(founds)

            zero = jnp.zeros((8, LANES), jnp.float32)
            carry = list(lax.fori_loop(0, whole, sweep, (zero,) * 8))
            for j, value in enumerate(tail):
                start = whole * 8 * NET + 8 * j
                total = carry[j % 4] + jnp.exp(value - peak)
                hit = wanted == start
                if start + 8 > width:
                    hit = hit & (sub < width - start)
                carry[j % 4], carry[4 + j % 4] = total, carry[4 + j % 4] + jnp.where(hit, value, 0.0)
            total = carry[0] + carry[1] + carry[2] + carry[3]
            found = carry[4] + carry[5] + carry[6] + carry[7]
            for k in range(TOPK):
                stat_ref[k : k + 1, :] = best[k][:1]
            stat_ref[TOPK : TOPK + 1, :] = jnp.sum(total, axis=0, keepdims=True)
            stat_ref[TOPK + 1 : TOPK + 2, :] = jnp.sum(found, axis=0, keepdims=True)
            turned = stat_ref[...].T
            for j in range(LANES // each):
                out_ref[owner_ref[lane // each + j]] = turned[j * each : (j + 1) * each]


def head(owner, near, far, w, ids, tile=680):
    half, depth = near.shape
    rows = 2 * half
    width = w.shape[1]
    devices = owner.shape[0]
    steps = -(-width // tile)
    return pl.pallas_call(
        functools.partial(head_kernel, steps=steps, width=width),
        grid_spec=pltpu.PrefetchScalarGridSpec(
            num_scalar_prefetch=1,
            grid=(steps,),
            in_specs=[
                pl.BlockSpec((half, depth), lambda i, o: (0, 0)),
                pl.BlockSpec((half, depth), lambda i, o: (0, 0)),
                pl.BlockSpec((tile, depth), lambda i, o: (i, 0)),
                pl.BlockSpec((1, rows), lambda i, o: (0, 0)),
            ],
            out_specs=pl.BlockSpec((devices, rows // devices, LANES), lambda i, o: (0, 0, 0)),
            scratch_shapes=[
                pltpu.VMEM((rows, depth), jnp.bfloat16),
                pltpu.VMEM((steps * tile, rows), jnp.float32),
                pltpu.VMEM((LANES, LANES), jnp.float32),
            ],
        ),
        out_shape=jax.ShapeDtypeStruct((devices, rows // devices, LANES), jnp.float32),
        cost_estimate=pl.CostEstimate(
            flops=2 * rows * depth * width, bytes_accessed=2 * depth * (width + rows), transcendentals=rows * width
        ),
        name="head",
    )(owner, near, far, w.T, ids)


def finish_kernel(*refs, batches):
    stats, seq_ref, (lp_ref, norm_ref, mass_ref, seq_out) = refs[:batches], refs[batches], refs[batches + 1 :]
    each = stats[0].shape[1]
    sources = stats[0].shape[0]
    lane = lax.broadcasted_iota(jnp.int32, (each, LANES), 1)
    row = lax.broadcasted_iota(jnp.int32, (each, LANES), 0)
    seq_row = lax.broadcasted_iota(jnp.int32, (SEQS, LANES), 0)
    seq_lane = lax.broadcasted_iota(jnp.int32, (SEQS, LANES), 1)

    def across(column):
        return jnp.sum(jnp.where(lane == row, column, 0.0), axis=0, keepdims=True)

    partial = jnp.zeros((1, LANES), jnp.float32)
    for m in range(batches):
        values = [stats[m][s] for s in range(sources)]
        pool = [jnp.where(lane < TOPK, v, -jnp.inf) for v in values]
        best = pool[0]
        for v in pool[1:]:
            best = jnp.maximum(best, v)
        peak = jnp.max(best, axis=1, keepdims=True)
        total = jnp.zeros((each, LANES), jnp.float32)
        found = jnp.zeros((each, LANES), jnp.float32)
        for v in values:
            total = total + v * jnp.exp(v[:, :1] - peak)
            found = found + v
        log_norm = peak + jnp.log(total[:, TOPK : TOPK + 1])
        token = found[:, TOPK + 1 : TOPK + 2] - log_norm
        left = jnp.full((each, 1), float(TOPK), jnp.float32)
        mass = jnp.zeros((each, 1), jnp.float32)
        top = peak
        for k in range(TOPK):
            hits = jnp.zeros((each, LANES), jnp.float32)
            for v in pool:
                hits = hits + jnp.where(v == top, 1.0, 0.0)
            count = jnp.minimum(jnp.sum(hits, axis=1, keepdims=True), left)
            mass = mass + jnp.where(count > 0.0, count * jnp.exp(top - log_norm), 0.0)
            left = left - count
            if k + 1 < TOPK:
                best = jnp.full((each, LANES), -jnp.inf, jnp.float32)
                for v in pool:
                    best = jnp.maximum(best, jnp.where(v < top, v, -jnp.inf))
                top = jnp.max(best, axis=1, keepdims=True)
        token_row = across(token)
        lp_ref[m : m + 1, :] = token_row
        norm_ref[m : m + 1, :] = across(log_norm)
        mass_ref[m : m + 1, :] = across(mass)
        ids = jnp.broadcast_to(seq_ref[m : m + 1, :], (SEQS, LANES))
        chosen = jnp.where(ids == seq_row, jnp.broadcast_to(token_row, (SEQS, LANES)), 0.0)
        sums = jnp.sum(chosen, axis=1, keepdims=True)
        partial = partial + jnp.sum(jnp.where(seq_lane == seq_row + m * SEQS, sums, 0.0), axis=0, keepdims=True)
    seq_out[...] = jnp.broadcast_to(partial[None], seq_out.shape)


def finish(stats, seq_ids):
    batches, each = seq_ids.shape
    devices = stats[0].shape[0]
    padded = jnp.pad(seq_ids, ((0, 0), (0, LANES - each)), constant_values=-1)
    row = jax.ShapeDtypeStruct((batches, LANES), jnp.float32)
    lp, norm, mass, seq = pl.pallas_call(
        functools.partial(finish_kernel, batches=batches),
        out_shape=(row, row, row, jax.ShapeDtypeStruct((devices, 1, LANES), jnp.float32)),
        name="finish",
    )(*stats, padded)
    return lp[:, :each], norm[:, :each], mass[:, :each], seq


def body(hidden_in, gain_ffn, w_gate, w_up, w_down, gain_final, head_weight, sampled_ids, seq_ids):
    batches, each, width = hidden_in.shape
    size = lax.axis_size("vocab")
    devices = 2 * size
    section = lax.axis_index("section")
    place = lax.axis_index("vocab")
    owner = block_owner(size, section, place)
    first_column = (section * size + place) * head_weight.shape[1]
    ids = sampled_ids.reshape(batches, devices, each)[:, owner].reshape(batches, 1, devices * each) - first_column
    gathered = [gather_rows(rms_norm(hidden_in[m].astype(jnp.float32), gain_ffn), size) for m in range(batches)]
    stats = []
    for m in range(batches):
        branch = scatter_sum(*ffn(*gathered[m], w_gate, w_up, w_down), size)
        residual = (hidden_in[m].astype(jnp.float32) + branch).astype(jnp.bfloat16)
        scaled = rms_norm(residual.astype(jnp.float32), gain_final)
        stats.append(head(owner, *gather_rows(scaled, size), head_weight, ids[m]))
    received = lax.all_to_all(jnp.concatenate(stats, axis=1), AXES, split_axis=0, concat_axis=0, tiled=True)
    received = [received[:, m * each : (m + 1) * each] for m in range(batches)]
    token_logprob, log_norm, top_mass, partial = finish(received, seq_ids)
    sums = jnp.sum(lax.all_to_all(partial, AXES, split_axis=0, concat_axis=0, tiled=True), axis=(0, 1))
    return token_logprob, log_norm, top_mass, sums[: batches * SEQS].reshape(batches, SEQS)


def solution(mesh):
    in_specs = (
        P(None, AXES, None),
        P(),
        P(None, AXES),
        P(None, AXES),
        P(AXES, None),
        P(),
        P(None, AXES),
        P(),
        P(None, AXES),
    )
    out_specs = (P(None, AXES), P(None, AXES), P(None, AXES), P())
    return jax.shard_map(body, mesh=mesh, in_specs=in_specs, out_specs=out_specs, check_vma=False)
```

```python
import functools

import jax
import jax.numpy as jnp
from jax import lax
from jax.experimental import pallas as pl
from jax.experimental.pallas import tpu as pltpu
from jax.sharding import PartitionSpec as P


SEQS = 8
TOPK = 20
LANES = 128
NET = 32
FFN_VMEM = 40 << 20
HEAD_VMEM = 40 << 20
AXES = ("section", "vocab")
epsilon = 1e-06


def rms_norm(wide, gain):
    square_mean = jnp.mean(wide * wide, axis=-1, keepdims=True)
    return (wide * lax.rsqrt(square_mean + epsilon) * gain).astype(jnp.bfloat16)


def close_kernel(own_ref, kept_ref, came_ref, gain_ref, out_ref):
    branch = kept_ref[...].astype(jnp.float32) + came_ref[...].astype(jnp.float32)
    residual = (own_ref[0].astype(jnp.float32) + branch).astype(jnp.bfloat16)
    out_ref[...] = rms_norm(residual.astype(jnp.float32), gain_ref[...])


def close_block(hidden_in, m, kept, came, gain):
    _, each, width = hidden_in.shape
    whole = pl.BlockSpec((each, width), lambda i: (0, 0))
    return pl.pallas_call(
        close_kernel,
        grid=(1,),
        in_specs=[
            pl.BlockSpec((1, each, width), lambda i: (m, 0, 0)),
            whole,
            whole,
            pl.BlockSpec((1, width), lambda i: (0, 0)),
        ],
        out_specs=whole,
        out_shape=jax.ShapeDtypeStruct((each, width), jnp.bfloat16),
        compiler_params=pltpu.CompilerParams(vmem_limit_bytes=4 << 20),
        cost_estimate=pl.CostEstimate(flops=8 * each * width, bytes_accessed=8 * each * width, transcendentals=0),
        name="close",
    )(hidden_in, kept, came, gain.reshape(1, width))


def step_masks(size):
    bits = [1 << b for b in reversed(range(size.bit_length() - 1))]
    return bits, bits[:-2] + [bits[-1], bits[-2]]


def step_perms(size):
    first, second = step_masks(size)
    return [
        [(s * size + i, s * size + (i ^ mask)) for s, mask in enumerate(pair) for i in range(size)]
        for pair in zip(first, second)
    ]


def core_perm(size):
    return [(s * size + i, (1 - s) * size + i) for s in range(2) for i in range(size)]


def move(rows, perm):
    return lax.ppermute(rows, AXES, perm)


def gather_rows(rows, size):
    held = rows
    for perm in step_perms(size):
        held = jnp.concatenate([held, move(held, perm)], axis=0)
    return held, move(held, core_perm(size))


def scatter_sum(near, far, size):
    held = near + move(far, core_perm(size))
    perms = step_perms(size)
    for j in reversed(range(1, len(perms))):
        half = held.shape[0] // 2
        held = held[:half] + move(held[half:], perms[j])
    half = held.shape[0] // 2
    return held[:half], move(held[half:], perms[0])


def block_owner(size, section, place):
    tables = []
    for masks in step_masks(size):
        table = []
        for q in range(size):
            mask = 0
            for j, m in enumerate(masks):
                if q >> j & 1:
                    mask ^= m
            table.append(mask)
        tables.append(jnp.array(table, jnp.int32))
    mine = jnp.where(section == 0, tables[0], tables[1])
    other = jnp.where(section == 0, tables[1], tables[0])
    return jnp.concatenate([section * size + (place ^ mine), (1 - section) * size + (place ^ other)])


def turned_dot(a, b):
    return lax.dot_general(a, b, (((1,), (1,)), ((), ())), preferred_element_type=jnp.float32)


def ffn_kernel(near_ref, far_ref, wg_ref, wu_ref, wd_ref, near_out, far_out, x_ref, turned_ref, h_ref, *, steps):
    i = pl.program_id(0)
    half = near_ref.shape[0]
    tile = wg_ref.shape[0]

    @pl.when(i == 0)
    def _():
        x_ref[:half] = near_ref[...]
        x_ref[half:] = far_ref[...]

    @pl.when(i < steps)
    def _():
        gate = turned_dot(wg_ref[...], x_ref[...])
        up = turned_dot(wu_ref[...], x_ref[...])
        turned_ref[pl.ds(pl.multiple_of(i * tile, tile), tile), :] = gate / (1.0 + jnp.exp(-gate)) * up

    @pl.when(i == steps - 1)
    def _():
        h_ref[...] = turned_ref[...].T.astype(jnp.bfloat16)

    @pl.when(i >= steps)
    def _():
        part = jnp.dot(h_ref[...], wd_ref[...], preferred_element_type=jnp.float32).astype(near_out.dtype)
        near_out[...] = part[:half]
        far_out[...] = part[half:]


def ffn(near, far, w_gate, w_up, w_down):
    half, width = near.shape
    rows = 2 * half
    hidden = w_gate.shape[1]
    tile = hidden // 2 if hidden % 32 == 0 else hidden
    block = 1792 if width % 1792 == 0 else width
    steps = hidden // tile

    def first(i):
        return jnp.minimum(i, steps - 1)

    def second(i):
        return jnp.maximum(i - steps, 0)

    part = jax.ShapeDtypeStruct((half, width), jnp.bfloat16)
    return pl.pallas_call(
        functools.partial(ffn_kernel, steps=steps),
        grid=(steps + width // block,),
        in_specs=[
            pl.BlockSpec((half, width), lambda i: (0, 0), pipeline_mode=pl.Buffered(1)),
            pl.BlockSpec((half, width), lambda i: (0, 0), pipeline_mode=pl.Buffered(1)),
            pl.BlockSpec((tile, width), lambda i: (first(i), 0)),
            pl.BlockSpec((tile, width), lambda i: (first(i), 0)),
            pl.BlockSpec((hidden, block), lambda i: (0, second(i))),
        ],
        out_specs=[pl.BlockSpec((half, block), lambda i: (0, second(i)))] * 2,
        out_shape=(part, part),
        scratch_shapes=[
            pltpu.VMEM((rows, width), jnp.bfloat16),
            pltpu.VMEM((hidden, rows), jnp.float32),
            pltpu.VMEM((rows, hidden), jnp.bfloat16),
        ],
        cost_estimate=pl.CostEstimate(
            flops=6 * rows * width * hidden, bytes_accessed=2 * width * (3 * hidden + 2 * rows), transcendentals=0
        ),
        compiler_params=pltpu.CompilerParams(vmem_limit_bytes=FFN_VMEM),
        name="ffn",
    )(near, far, w_gate.T, w_up.T, w_down)


def pair(values, i, j):
    a, b = values[i], values[j]
    if b is None:
        return
    if a is None:
        values[i], values[j] = b, None
    else:
        values[i], values[j] = jnp.maximum(a, b), jnp.minimum(a, b)


def sort_net(values):
    values = list(values) + [None] * (NET - len(values))
    p = 1
    while p < NET:
        k = p
        while k >= 1:
            for j in range(k % p, NET - k, 2 * k):
                for i in range(min(k, NET - j - k)):
                    if (i + j) // (2 * p) == (i + j + k) // (2 * p):
                        pair(values, i + j, i + j + k)
            k //= 2
        p *= 2
    return values[:TOPK]


def merge_net(a, b):
    a = list(a) + [None] * (NET - len(a))
    b = list(b) + [None] * (NET - len(b))
    c = []
    for x, y in zip(a, reversed(b)):
        c.append(y if x is None else x if y is None else jnp.maximum(x, y))
    k = NET // 2
    while k >= 1:
        for base in range(0, NET, 2 * k):
            for i in range(base, base + k):
                pair(c, i, i + k)
        k //= 2
    return c[:TOPK]


def head_kernel(
    owner_ref, near_ref, far_ref, w_ref, ids_ref, seq_ref, out_ref, x_ref, logits_ref, stat_ref, table_ref, pack_ref,
    *, steps, width, each
):
    i = pl.program_id(0)
    half = near_ref.shape[0]
    tile = w_ref.shape[0]

    @pl.when(i == 0)
    def _():
        x_ref[:half] = near_ref[...]
        x_ref[half:] = far_ref[...]

    logits_ref[pl.ds(pl.multiple_of(i * tile, tile), tile), :] = turned_dot(w_ref[...], x_ref[...])

    @pl.when(i == steps - 1)
    def _():
        rows = x_ref.shape[0]
        groups = rows // LANES
        whole = width // (8 * NET)
        sub = lax.broadcasted_iota(jnp.int32, (8, LANES), 0)

        def load(start, lanes):
            return logits_ref[pl.ds(start, 8), lanes]

        def rest(lanes):
            values = []
            for start in range(whole * 8 * NET, width, 8):
                value = load(start, lanes)
                if start + 8 > width:
                    value = jnp.where(sub < width - start, value, -jnp.inf)
                values.append(value)
            return values

        stat_ref[...] = jnp.zeros_like(stat_ref)
        for lane in range(0, rows, LANES):
            lanes = slice(lane, lane + LANES)

            def collect(g, best):
                start = pl.multiple_of(g * 8 * NET, 8 * NET)
                return tuple(merge_net(best, sort_net([load(start + 8 * j, lanes) for j in range(NET)])))

            low = jnp.full((8, LANES), -jnp.inf, jnp.float32)
            best = list(lax.fori_loop(0, whole, collect, (low,) * TOPK))
            tail = rest(lanes)
            if tail:
                ranked = sort_net(tail)
                best = merge_net(best, [r for r in ranked if r is not None])
            for shift in (4, 2, 1):
                best = merge_net(best, [pltpu.roll(b, shift, 0) for b in best])
            peak = best[0]
            wanted = jnp.broadcast_to(ids_ref[:, lanes], (8, LANES)) - sub

            def scan(value, start, total, found):
                total = total + jnp.exp(value - peak)
                return total, found + jnp.where(wanted == start, value, 0.0)

            def sweep(g, carry):
                start = pl.multiple_of(g * 8 * NET, 8 * NET)
                totals, founds = list(carry[:4]), list(carry[4:])
                for j in range(NET):
                    t, f = scan(load(start + 8 * j, lanes), start + 8 * j, totals[j % 4], founds[j % 4])
                    totals[j % 4], founds[j % 4] = t, f
                return tuple(totals) + tuple(founds)

            zero = jnp.zeros((8, LANES), jnp.float32)
            carry = list(lax.fori_loop(0, whole, sweep, (zero,) * 8))
            for j, value in enumerate(tail):
                start = whole * 8 * NET + 8 * j
                total = carry[j % 4] + jnp.exp(value - peak)
                hit = wanted == start
                if start + 8 > width:
                    hit = hit & (sub < width - start)
                carry[j % 4], carry[4 + j % 4] = total, carry[4 + j % 4] + jnp.where(hit, value, 0.0)
            total = carry[0] + carry[1] + carry[2] + carry[3]
            found = carry[4] + carry[5] + carry[6] + carry[7]
            for k in range(TOPK):
                stat_ref[k : k + 1, :] = best[k][:1]
            stat_ref[TOPK : TOPK + 1, :] = jnp.sum(total, axis=0, keepdims=True)
            stat_ref[TOPK + 1 : TOPK + 2, :] = jnp.sum(found, axis=0, keepdims=True)
            turned = stat_ref[...].T
            for j in range(LANES // each):
                owner = owner_ref[lane // each + j]
                block = turned[j * each : (j + 1) * each]
                out_ref[owner, :each, :] = block
                start = owner * each if each % 8 else pl.multiple_of(owner * each, 8)
                table_ref[pl.ds(start, each), :] = block
        for g in range(groups):
            turned = table_ref[g * LANES : (g + 1) * LANES, :].T
            for k, entry in enumerate((0, TOPK, TOPK + 1)):
                pack_ref[k * groups + g : k * groups + g + 1, :] = turned[entry : entry + 1]
            pack_ref[3 * groups + g : 3 * groups + g + 1, :] = seq_ref[g : g + 1, :]
        out_ref[:, each:, :] = jnp.broadcast_to(pack_ref[...][None], (out_ref.shape[0],) + pack_ref.shape)


def head(owner, near, far, w, ids, seq, tile=680):
    half, depth = near.shape
    rows = 2 * half
    width = w.shape[1]
    devices = owner.shape[0]
    each = rows // devices
    groups = rows // LANES
    packed = -(-4 * groups // 8) * 8
    steps = -(-width // tile)
    return pl.pallas_call(
        functools.partial(head_kernel, steps=steps, width=width, each=each),
        grid_spec=pltpu.PrefetchScalarGridSpec(
            num_scalar_prefetch=1,
            grid=(steps,),
            in_specs=[
                pl.BlockSpec((half, depth), lambda i, o: (0, 0), pipeline_mode=pl.Buffered(1)),
                pl.BlockSpec((half, depth), lambda i, o: (0, 0), pipeline_mode=pl.Buffered(1)),
                pl.BlockSpec((tile, depth), lambda i, o: (i, 0)),
                pl.BlockSpec((1, rows), lambda i, o: (0, 0)),
                pl.BlockSpec((groups, LANES), lambda i, o: (0, 0)),
            ],
            out_specs=pl.BlockSpec((devices, each + packed, LANES), lambda i, o: (0, 0, 0)),
            scratch_shapes=[
                pltpu.VMEM((rows, depth), jnp.bfloat16),
                pltpu.VMEM((steps * tile, rows), jnp.float32),
                pltpu.VMEM((LANES, LANES), jnp.float32),
                pltpu.VMEM((rows, LANES), jnp.float32),
                pltpu.VMEM((packed, LANES), jnp.float32),
            ],
        ),
        out_shape=jax.ShapeDtypeStruct((devices, each + packed, LANES), jnp.float32),
        cost_estimate=pl.CostEstimate(
            flops=2 * rows * depth * width, bytes_accessed=2 * depth * (width + rows), transcendentals=rows * width
        ),
        compiler_params=pltpu.CompilerParams(vmem_limit_bytes=HEAD_VMEM),
        name="head",
    )(owner, near, far, w.T, ids, seq)


def finish_kernel(*refs, batches, each, groups):
    stats, (lp_ref, norm_ref, mass_ref, seq_out) = refs[:batches], refs[batches:]
    sources = stats[0].shape[0]
    lane = lax.broadcasted_iota(jnp.int32, (each, LANES), 1)
    row = lax.broadcasted_iota(jnp.int32, (each, LANES), 0)
    seq_row = lax.broadcasted_iota(jnp.int32, (SEQS, LANES), 0).astype(jnp.float32)
    seq_lane = lax.broadcasted_iota(jnp.int32, (SEQS, LANES), 1)
    seq_place = lax.broadcasted_iota(jnp.int32, (SEQS, LANES), 0)

    def across(column):
        return jnp.sum(jnp.where(lane == row, column, 0.0), axis=0, keepdims=True)

    for m in range(batches):
        values = [stats[m][s, :each] for s in range(sources)]
        pool = [jnp.where(lane < TOPK, v, -jnp.inf) for v in values]
        best = pool[0]
        for v in pool[1:]:
            best = jnp.maximum(best, v)
        peak = jnp.max(best, axis=1, keepdims=True)
        total = jnp.zeros((each, LANES), jnp.float32)
        found = jnp.zeros((each, LANES), jnp.float32)
        for v in values:
            total = total + v * jnp.exp(v[:, :1] - peak)
            found = found + v
        log_norm = peak + jnp.log(total[:, TOPK : TOPK + 1])
        token = found[:, TOPK + 1 : TOPK + 2] - log_norm
        left = jnp.full((each, 1), float(TOPK), jnp.float32)
        mass = jnp.zeros((each, 1), jnp.float32)
        top = peak
        for k in range(TOPK):
            hits = jnp.zeros((each, LANES), jnp.float32)
            for v in pool:
                hits = hits + jnp.where(v == top, 1.0, 0.0)
            count = jnp.minimum(jnp.sum(hits, axis=1, keepdims=True), left)
            mass = mass + jnp.where(count > 0.0, count * jnp.exp(top - log_norm), 0.0)
            left = left - count
            if k + 1 < TOPK:
                best = jnp.full((each, LANES), -jnp.inf, jnp.float32)
                for v in pool:
                    best = jnp.maximum(best, jnp.where(v < top, v, -jnp.inf))
                top = jnp.max(best, axis=1, keepdims=True)
        lp_ref[m : m + 1, :] = across(token)
        norm_ref[m : m + 1, :] = across(log_norm)
        mass_ref[m : m + 1, :] = across(mass)
        packs = [stats[m][s, each:] for s in range(sources)]
        highest = packs[0]
        for v in packs[1:]:
            highest = jnp.maximum(highest, v)
        total = jnp.zeros_like(highest)
        found = jnp.zeros_like(highest)
        for v in packs:
            total = total + v * pltpu.roll(jnp.exp(v - highest), groups, 0)
            found = found + v
        sums = jnp.zeros((SEQS, 1), jnp.float32)
        for g in range(groups):
            norm = highest[g : g + 1] + jnp.log(total[groups + g : groups + g + 1])
            token_row = found[2 * groups + g : 2 * groups + g + 1] - norm
            ids = jnp.broadcast_to(found[3 * groups + g : 3 * groups + g + 1], (SEQS, LANES))
            chosen = jnp.where(ids == seq_row, jnp.broadcast_to(token_row, (SEQS, LANES)), 0.0)
            sums = sums + jnp.sum(chosen, axis=1, keepdims=True)
        seq_out[m : m + 1, :] = jnp.sum(jnp.where(seq_lane == seq_place, sums, 0.0), axis=0, keepdims=True)


def finish(stats, each, groups):
    batches = len(stats)
    row = jax.ShapeDtypeStruct((batches, LANES), jnp.float32)
    lp, norm, mass, seq = pl.pallas_call(
        functools.partial(finish_kernel, batches=batches, each=each, groups=groups),
        out_shape=(row, row, row, row),
        name="finish",
    )(*stats)
    return lp[:, :each], norm[:, :each], mass[:, :each], seq[:, :SEQS]


def score(hidden_in, gain_ffn, w_gate, w_up, w_down, gain_final, head_weight, sampled_ids, seq_ids):
    batches, each, _ = hidden_in.shape
    size = lax.axis_size("vocab")
    devices = 2 * size
    section = lax.axis_index("section")
    place = lax.axis_index("vocab")
    owner = block_owner(size, section, place)
    first_column = (section * size + place) * head_weight.shape[1]
    ids = sampled_ids.reshape(batches, devices, each)[:, owner].reshape(batches, 1, devices * each) - first_column
    groups = devices * each // LANES
    own = jnp.arange(devices)[None, :, None] == section * size + place
    seq = jnp.where(own, seq_ids[:, None, :].astype(jnp.float32), 0.0).reshape(batches, groups, LANES)
    gathered = [gather_rows(rms_norm(hidden_in[m].astype(jnp.float32), gain_ffn), size) for m in range(batches)]
    stats = []
    for m in range(batches):
        parts = ffn(*gathered[m], w_gate, w_up, w_down)
        kept, came = scatter_sum(*parts, size)
        scaled = close_block(hidden_in, m, kept, came, gain_final)
        spread = gather_rows(scaled, size)
        part = head(owner, *spread, head_weight, ids[m], seq[m])
        stats.append(lax.all_to_all(part, AXES, split_axis=0, concat_axis=0, tiled=True))
    return finish(stats, each, groups)


def solution(mesh):
    in_specs = (
        P(None, AXES, None),
        P(),
        P(None, AXES),
        P(None, AXES),
        P(AXES, None),
        P(),
        P(None, AXES),
        P(),
        P(None, AXES),
    )
    out_specs = (P(None, AXES), P(None, AXES), P(None, AXES), P())
    return jax.shard_map(score, mesh=mesh, in_specs=in_specs, out_specs=out_specs, check_vma=False)
```

```python
import functools

import jax
import jax.numpy as jnp
from jax import lax
from jax.experimental import pallas as pl
from jax.experimental.pallas import tpu as pltpu
from jax.sharding import PartitionSpec as P


SEQS = 8
TOPK = 20
LANES = 128
NET = 32
FFN_VMEM = 40 << 20
HEAD_VMEM = 40 << 20
HEAD_TILE = 680
AXES = ("section", "vocab")
epsilon = 1e-06


def rms_norm(wide, gain):
    square_mean = jnp.mean(wide * wide, axis=-1, keepdims=True)
    return (wide * lax.rsqrt(square_mean + epsilon) * gain).astype(jnp.bfloat16)


def close_kernel(own_ref, kept_ref, came_ref, gain_ref, out_ref):
    branch = kept_ref[...].astype(jnp.float32) + came_ref[...].astype(jnp.float32)
    residual = (own_ref[0].astype(jnp.float32) + branch).astype(jnp.bfloat16)
    out_ref[...] = rms_norm(residual.astype(jnp.float32), gain_ref[...])


def close_block(hidden_in, m, kept, came, gain):
    _, each, width = hidden_in.shape
    whole = pl.BlockSpec((each, width), lambda i: (0, 0))
    return pl.pallas_call(
        close_kernel,
        grid=(1,),
        in_specs=[
            pl.BlockSpec((1, each, width), lambda i: (m, 0, 0)),
            whole,
            whole,
            pl.BlockSpec((1, width), lambda i: (0, 0)),
        ],
        out_specs=whole,
        out_shape=jax.ShapeDtypeStruct((each, width), jnp.bfloat16),
        compiler_params=pltpu.CompilerParams(vmem_limit_bytes=4 << 20),
        cost_estimate=pl.CostEstimate(flops=8 * each * width, bytes_accessed=8 * each * width, transcendentals=0),
        name="close",
    )(hidden_in, kept, came, gain.reshape(1, width))


def step_masks(size):
    bits = [1 << b for b in reversed(range(size.bit_length() - 1))]
    return bits, bits[:-2] + [bits[-1], bits[-2]]


def step_perms(size):
    first, second = step_masks(size)
    return [
        [(s * size + i, s * size + (i ^ mask)) for s, mask in enumerate(pair) for i in range(size)]
        for pair in zip(first, second)
    ]


def core_perm(size):
    return [(s * size + i, (1 - s) * size + i) for s in range(2) for i in range(size)]


def move(rows, perm):
    return lax.ppermute(rows, AXES, perm)


def gather_rows(rows, size):
    held = rows
    for perm in step_perms(size):
        held = jnp.concatenate([held, move(held, perm)], axis=0)
    return held, move(held, core_perm(size))


def scatter_sum(near, far, size):
    held = near + move(far, core_perm(size))
    perms = step_perms(size)
    for j in reversed(range(1, len(perms))):
        half = held.shape[0] // 2
        held = held[:half] + move(held[half:], perms[j])
    half = held.shape[0] // 2
    return held[:half], move(held[half:], perms[0])


def block_owner(size, section, place):
    tables = []
    for masks in step_masks(size):
        table = []
        for q in range(size):
            mask = 0
            for j, m in enumerate(masks):
                if q >> j & 1:
                    mask ^= m
            table.append(mask)
        tables.append(jnp.array(table, jnp.int32))
    mine = jnp.where(section == 0, tables[0], tables[1])
    other = jnp.where(section == 0, tables[1], tables[0])
    return jnp.concatenate([section * size + (place ^ mine), (1 - section) * size + (place ^ other)])


def turned_dot(a, b):
    return lax.dot_general(a, b, (((1,), (1,)), ((), ())), preferred_element_type=jnp.float32)


def ffn_kernel(near_ref, far_ref, wg_ref, wu_ref, wd_ref, near_out, far_out, x_ref, turned_ref, h_ref, *, steps):
    i = pl.program_id(0)
    half = near_ref.shape[0]
    tile = wg_ref.shape[0]

    @pl.when(i == 0)
    def _():
        x_ref[:half] = near_ref[...]
        x_ref[half:] = far_ref[...]

    @pl.when(i < steps)
    def _():
        gate = turned_dot(wg_ref[...], x_ref[...])
        up = turned_dot(wu_ref[...], x_ref[...])
        turned_ref[pl.ds(pl.multiple_of(i * tile, tile), tile), :] = gate / (1.0 + jnp.exp(-gate)) * up

    @pl.when(i == steps - 1)
    def _():
        h_ref[...] = turned_ref[...].T.astype(jnp.bfloat16)

    @pl.when(i >= steps)
    def _():
        part = jnp.dot(h_ref[...], wd_ref[...], preferred_element_type=jnp.float32).astype(near_out.dtype)
        near_out[...] = part[:half]
        far_out[...] = part[half:]


def ffn(near, far, w_gate, w_up, w_down):
    half, width = near.shape
    rows = 2 * half
    hidden = w_gate.shape[1]
    tile = hidden // 2 if hidden % 32 == 0 else hidden
    block = 1792 if width % 1792 == 0 else width
    steps = hidden // tile

    def first(i):
        return jnp.minimum(i, steps - 1)

    def second(i):
        return jnp.maximum(i - steps, 0)

    part = jax.ShapeDtypeStruct((half, width), jnp.bfloat16)
    return pl.pallas_call(
        functools.partial(ffn_kernel, steps=steps),
        grid=(steps + width // block,),
        in_specs=[
            pl.BlockSpec((half, width), lambda i: (0, 0), pipeline_mode=pl.Buffered(1)),
            pl.BlockSpec((half, width), lambda i: (0, 0), pipeline_mode=pl.Buffered(1)),
            pl.BlockSpec((tile, width), lambda i: (first(i), 0)),
            pl.BlockSpec((tile, width), lambda i: (first(i), 0)),
            pl.BlockSpec((hidden, block), lambda i: (0, second(i))),
        ],
        out_specs=[pl.BlockSpec((half, block), lambda i: (0, second(i)))] * 2,
        out_shape=(part, part),
        scratch_shapes=[
            pltpu.VMEM((rows, width), jnp.bfloat16),
            pltpu.VMEM((hidden, rows), jnp.float32),
            pltpu.VMEM((rows, hidden), jnp.bfloat16),
        ],
        cost_estimate=pl.CostEstimate(
            flops=6 * rows * width * hidden, bytes_accessed=2 * width * (3 * hidden + 2 * rows), transcendentals=0
        ),
        compiler_params=pltpu.CompilerParams(vmem_limit_bytes=FFN_VMEM),
        name="ffn",
    )(near, far, w_gate.T, w_up.T, w_down)


def pair(values, i, j):
    a, b = values[i], values[j]
    if b is None:
        return
    if a is None:
        values[i], values[j] = b, None
    else:
        values[i], values[j] = jnp.maximum(a, b), jnp.minimum(a, b)


def sort_net(values):
    values = list(values) + [None] * (NET - len(values))
    p = 1
    while p < NET:
        k = p
        while k >= 1:
            for j in range(k % p, NET - k, 2 * k):
                for i in range(min(k, NET - j - k)):
                    if (i + j) // (2 * p) == (i + j + k) // (2 * p):
                        pair(values, i + j, i + j + k)
            k //= 2
        p *= 2
    return values[:TOPK]


def merge_net(a, b):
    a = list(a) + [None] * (NET - len(a))
    b = list(b) + [None] * (NET - len(b))
    c = []
    for x, y in zip(a, reversed(b)):
        c.append(y if x is None else x if y is None else jnp.maximum(x, y))
    k = NET // 2
    while k >= 1:
        for base in range(0, NET, 2 * k):
            for i in range(base, base + k):
                pair(c, i, i + k)
        k //= 2
    return c[:TOPK]


def early_kernel(near_ref, far_ref, w_ref, out_ref, x_ref):
    half = near_ref.shape[0]

    @pl.when(pl.program_id(0) == 0)
    def _():
        x_ref[:half] = near_ref[...]
        x_ref[half:] = far_ref[...]

    out_ref[...] = turned_dot(w_ref[...], x_ref[...])


def early_head(near, far, w, steps, tile=HEAD_TILE):
    half, depth = near.shape
    rows = 2 * half
    return pl.pallas_call(
        early_kernel,
        grid=(steps,),
        in_specs=[
            pl.BlockSpec((half, depth), lambda i: (0, 0), pipeline_mode=pl.Buffered(1)),
            pl.BlockSpec((half, depth), lambda i: (0, 0), pipeline_mode=pl.Buffered(1)),
            pl.BlockSpec((tile, depth), lambda i: (i, 0)),
        ],
        out_specs=pl.BlockSpec((tile, rows), lambda i: (i, 0)),
        out_shape=jax.ShapeDtypeStruct((steps * tile, rows), jnp.float32),
        scratch_shapes=[pltpu.VMEM((rows, depth), jnp.bfloat16)],
        cost_estimate=pl.CostEstimate(
            flops=2 * rows * depth * steps * tile, bytes_accessed=2 * depth * (steps * tile + rows), transcendentals=0
        ),
        compiler_params=pltpu.CompilerParams(vmem_limit_bytes=HEAD_VMEM),
        name="early_head",
    )(near, far, w.T)


def head_kernel(owner_ref, near_ref, far_ref, w_ref, ids_ref, seq_ref, *refs, steps, width, each, skip):
    early_refs, (out_ref, x_ref, logits_ref, stat_ref, table_ref, pack_ref) = refs[:-6], refs[-6:]
    i = pl.program_id(0)
    half = near_ref.shape[0]
    tile = w_ref.shape[0]

    @pl.when(i == 0)
    def _():
        x_ref[:half] = near_ref[...]
        x_ref[half:] = far_ref[...]
        for early_ref in early_refs:
            logits_ref[: early_ref.shape[0]] = early_ref[...]

    logits_ref[pl.ds(pl.multiple_of((i + skip) * tile, tile), tile), :] = turned_dot(w_ref[...], x_ref[...])

    @pl.when(i == steps - 1)
    def _():
        rows = x_ref.shape[0]
        groups = rows // LANES
        whole = width // (8 * NET)
        sub = lax.broadcasted_iota(jnp.int32, (8, LANES), 0)

        def load(start, lanes):
            return logits_ref[pl.ds(start, 8), lanes]

        def rest(lanes):
            values = []
            for start in range(whole * 8 * NET, width, 8):
                value = load(start, lanes)
                if start + 8 > width:
                    value = jnp.where(sub < width - start, value, -jnp.inf)
                values.append(value)
            return values

        stat_ref[...] = jnp.zeros_like(stat_ref)
        for lane in range(0, rows, LANES):
            lanes = slice(lane, lane + LANES)

            def collect(g, best):
                start = pl.multiple_of(g * 8 * NET, 8 * NET)
                return tuple(merge_net(best, sort_net([load(start + 8 * j, lanes) for j in range(NET)])))

            low = jnp.full((8, LANES), -jnp.inf, jnp.float32)
            best = list(lax.fori_loop(0, whole, collect, (low,) * TOPK))
            tail = rest(lanes)
            if tail:
                ranked = sort_net(tail)
                best = merge_net(best, [r for r in ranked if r is not None])
            for shift in (4, 2, 1):
                best = merge_net(best, [pltpu.roll(b, shift, 0) for b in best])
            peak = best[0]
            wanted = jnp.broadcast_to(ids_ref[:, lanes], (8, LANES)) - sub

            def scan(value, start, total, found):
                total = total + jnp.exp(value - peak)
                return total, found + jnp.where(wanted == start, value, 0.0)

            def sweep(g, carry):
                start = pl.multiple_of(g * 8 * NET, 8 * NET)
                totals, founds = list(carry[:4]), list(carry[4:])
                for j in range(NET):
                    t, f = scan(load(start + 8 * j, lanes), start + 8 * j, totals[j % 4], founds[j % 4])
                    totals[j % 4], founds[j % 4] = t, f
                return tuple(totals) + tuple(founds)

            zero = jnp.zeros((8, LANES), jnp.float32)
            carry = list(lax.fori_loop(0, whole, sweep, (zero,) * 8))
            for j, value in enumerate(tail):
                start = whole * 8 * NET + 8 * j
                total = carry[j % 4] + jnp.exp(value - peak)
                hit = wanted == start
                if start + 8 > width:
                    hit = hit & (sub < width - start)
                carry[j % 4], carry[4 + j % 4] = total, carry[4 + j % 4] + jnp.where(hit, value, 0.0)
            total = carry[0] + carry[1] + carry[2] + carry[3]
            found = carry[4] + carry[5] + carry[6] + carry[7]
            for k in range(TOPK):
                stat_ref[k : k + 1, :] = best[k][:1]
            stat_ref[TOPK : TOPK + 1, :] = jnp.sum(total, axis=0, keepdims=True)
            stat_ref[TOPK + 1 : TOPK + 2, :] = jnp.sum(found, axis=0, keepdims=True)
            turned = stat_ref[...].T
            for j in range(LANES // each):
                owner = owner_ref[lane // each + j]
                block = turned[j * each : (j + 1) * each]
                out_ref[owner, :each, :] = block
                start = owner * each if each % 8 else pl.multiple_of(owner * each, 8)
                table_ref[pl.ds(start, each), :] = block
        for g in range(groups):
            turned = table_ref[g * LANES : (g + 1) * LANES, :].T
            for k, entry in enumerate((0, TOPK, TOPK + 1)):
                pack_ref[k * groups + g : k * groups + g + 1, :] = turned[entry : entry + 1]
            pack_ref[3 * groups + g : 3 * groups + g + 1, :] = seq_ref[g : g + 1, :]
        out_ref[:, each:, :] = jnp.broadcast_to(pack_ref[...][None], (out_ref.shape[0],) + pack_ref.shape)


def head(owner, near, far, w, ids, seq, early=(), tile=HEAD_TILE):
    half, depth = near.shape
    rows = 2 * half
    width = w.shape[1]
    devices = owner.shape[0]
    each = rows // devices
    groups = rows // LANES
    packed = -(-4 * groups // 8) * 8
    skip = sum(e.shape[0] for e in early) // tile
    steps = -(-width // tile) - skip
    return pl.pallas_call(
        functools.partial(head_kernel, steps=steps, width=width, each=each, skip=skip),
        grid_spec=pltpu.PrefetchScalarGridSpec(
            num_scalar_prefetch=1,
            grid=(steps,),
            in_specs=[
                pl.BlockSpec((half, depth), lambda i, o: (0, 0), pipeline_mode=pl.Buffered(1)),
                pl.BlockSpec((half, depth), lambda i, o: (0, 0), pipeline_mode=pl.Buffered(1)),
                pl.BlockSpec((tile, depth), lambda i, o: (i + skip, 0)),
                pl.BlockSpec((1, rows), lambda i, o: (0, 0)),
                pl.BlockSpec((groups, LANES), lambda i, o: (0, 0)),
            ]
            + [pl.BlockSpec(e.shape, lambda i, o: (0, 0), pipeline_mode=pl.Buffered(1)) for e in early],
            out_specs=pl.BlockSpec((devices, each + packed, LANES), lambda i, o: (0, 0, 0)),
            scratch_shapes=[
                pltpu.VMEM((rows, depth), jnp.bfloat16),
                pltpu.VMEM(((steps + skip) * tile, rows), jnp.float32),
                pltpu.VMEM((LANES, LANES), jnp.float32),
                pltpu.VMEM((rows, LANES), jnp.float32),
                pltpu.VMEM((packed, LANES), jnp.float32),
            ],
        ),
        out_shape=jax.ShapeDtypeStruct((devices, each + packed, LANES), jnp.float32),
        cost_estimate=pl.CostEstimate(
            flops=2 * rows * depth * (width - skip * tile),
            bytes_accessed=2 * depth * (width - skip * tile + rows),
            transcendentals=rows * width,
        ),
        compiler_params=pltpu.CompilerParams(vmem_limit_bytes=HEAD_VMEM),
        name="head",
    )(owner, near, far, w.T, ids, seq, *early)


def finish_kernel(*refs, batches, each, groups):
    stats, (lp_ref, norm_ref, mass_ref, seq_out) = refs[:batches], refs[batches:]
    sources = stats[0].shape[0]
    lane = lax.broadcasted_iota(jnp.int32, (each, LANES), 1)
    row = lax.broadcasted_iota(jnp.int32, (each, LANES), 0)
    seq_row = lax.broadcasted_iota(jnp.int32, (SEQS, LANES), 0).astype(jnp.float32)
    seq_lane = lax.broadcasted_iota(jnp.int32, (SEQS, LANES), 1)
    seq_place = lax.broadcasted_iota(jnp.int32, (SEQS, LANES), 0)

    def across(column):
        return jnp.sum(jnp.where(lane == row, column, 0.0), axis=0, keepdims=True)

    for m in range(batches):
        values = [stats[m][s, :each] for s in range(sources)]
        pool = [jnp.where(lane < TOPK, v, -jnp.inf) for v in values]
        best = pool[0]
        for v in pool[1:]:
            best = jnp.maximum(best, v)
        peak = jnp.max(best, axis=1, keepdims=True)
        total = jnp.zeros((each, LANES), jnp.float32)
        found = jnp.zeros((each, LANES), jnp.float32)
        for v in values:
            total = total + v * jnp.exp(v[:, :1] - peak)
            found = found + v
        log_norm = peak + jnp.log(total[:, TOPK : TOPK + 1])
        token = found[:, TOPK + 1 : TOPK + 2] - log_norm
        left = jnp.full((each, 1), float(TOPK), jnp.float32)
        mass = jnp.zeros((each, 1), jnp.float32)
        top = peak
        for k in range(TOPK):
            hits = jnp.zeros((each, LANES), jnp.float32)
            for v in pool:
                hits = hits + jnp.where(v == top, 1.0, 0.0)
            count = jnp.minimum(jnp.sum(hits, axis=1, keepdims=True), left)
            mass = mass + jnp.where(count > 0.0, count * jnp.exp(top - log_norm), 0.0)
            left = left - count
            if k + 1 < TOPK:
                best = jnp.full((each, LANES), -jnp.inf, jnp.float32)
                for v in pool:
                    best = jnp.maximum(best, jnp.where(v < top, v, -jnp.inf))
                top = jnp.max(best, axis=1, keepdims=True)
        lp_ref[m : m + 1, :] = across(token)
        norm_ref[m : m + 1, :] = across(log_norm)
        mass_ref[m : m + 1, :] = across(mass)
        packs = [stats[m][s, each:] for s in range(sources)]
        highest = packs[0]
        for v in packs[1:]:
            highest = jnp.maximum(highest, v)
        total = jnp.zeros_like(highest)
        found = jnp.zeros_like(highest)
        for v in packs:
            total = total + v * pltpu.roll(jnp.exp(v - highest), groups, 0)
            found = found + v
        sums = jnp.zeros((SEQS, 1), jnp.float32)
        for g in range(groups):
            norm = highest[g : g + 1] + jnp.log(total[groups + g : groups + g + 1])
            token_row = found[2 * groups + g : 2 * groups + g + 1] - norm
            ids = jnp.broadcast_to(found[3 * groups + g : 3 * groups + g + 1], (SEQS, LANES))
            chosen = jnp.where(ids == seq_row, jnp.broadcast_to(token_row, (SEQS, LANES)), 0.0)
            sums = sums + jnp.sum(chosen, axis=1, keepdims=True)
        seq_out[m : m + 1, :] = jnp.sum(jnp.where(seq_lane == seq_place, sums, 0.0), axis=0, keepdims=True)


def finish(stats, each, groups):
    batches = len(stats)
    row = jax.ShapeDtypeStruct((batches, LANES), jnp.float32)
    lp, norm, mass, seq = pl.pallas_call(
        functools.partial(finish_kernel, batches=batches, each=each, groups=groups),
        out_shape=(row, row, row, row),
        name="finish",
    )(*stats)
    return lp[:, :each], norm[:, :each], mass[:, :each], seq[:, :SEQS]


def score(hidden_in, gain_ffn, w_gate, w_up, w_down, gain_final, head_weight, sampled_ids, seq_ids):
    batches, each, _ = hidden_in.shape
    size = lax.axis_size("vocab")
    devices = 2 * size
    section = lax.axis_index("section")
    place = lax.axis_index("vocab")
    owner = block_owner(size, section, place)
    first_column = (section * size + place) * head_weight.shape[1]
    ids = sampled_ids.reshape(batches, devices, each)[:, owner].reshape(batches, 1, devices * each) - first_column
    groups = devices * each // LANES
    own = jnp.arange(devices)[None, :, None] == section * size + place
    seq = jnp.where(own, seq_ids[:, None, :].astype(jnp.float32), 0.0).reshape(batches, groups, LANES)
    gathered = [gather_rows(rms_norm(hidden_in[m].astype(jnp.float32), gain_ffn), size) for m in range(batches)]
    stats = []
    for m in range(batches):
        parts = ffn(*gathered[m], w_gate, w_up, w_down)
        kept, came = scatter_sum(*parts, size)
        scaled = close_block(hidden_in, m, kept, came, gain_final)
        spread = gather_rows(scaled, size)
        early = ()
        steps = -(-head_weight.shape[1] // HEAD_TILE)
        if m + 1 < batches and steps > 1:
            early = (early_head(*spread, head_weight, steps // 2),)
        part = head(owner, *spread, head_weight, ids[m], seq[m], early)
        stats.append(lax.all_to_all(part, AXES, split_axis=0, concat_axis=0, tiled=True))
    return finish(stats, each, groups)


def solution(mesh):
    in_specs = (
        P(None, AXES, None),
        P(),
        P(None, AXES),
        P(None, AXES),
        P(AXES, None),
        P(),
        P(None, AXES),
        P(),
        P(None, AXES),
    )
    out_specs = (P(None, AXES), P(None, AXES), P(None, AXES), P())
    return jax.shard_map(score, mesh=mesh, in_specs=in_specs, out_specs=out_specs, check_vma=False)
```
